32 devices in a mesh: unit: 4 (over y, x), north: 4 (over z), east: 2 (over core).
Axes of the slice: x: 2, y: 2, z: 4, core: 2. Of those that a mesh axis runs over, the one named last changes fastest.
Arguments:
- pair_rows: bfloat16 [256, 64, 128], P(('unit', 'north'), 'east'), parts along dimension 0, may hold values from -6 to 6
- in_gain: float32 [128], replicated, may hold values from 0.25 to 1.75
- left_weight: bfloat16 [512, 128], P('unit'), parts along dimension 0, may hold values from -0.5 to 0.5
- right_weight: bfloat16 [512, 128], P('unit'), parts along dimension 0, may hold values from -0.5 to 0.5
- left_gate: bfloat16 [512, 128], P('unit'), parts along dimension 0, may hold values from -0.5 to 0.5
- right_gate: bfloat16 [512, 128], P('unit'), parts along dimension 0, may hold values from -0.5 to 0.5
- mid_gain: float32 [128], replicated, may hold values from 0.25 to 1.75
- out_weight: bfloat16 [512, 128], P('unit'), parts along dimension 0, may hold values from -0.5 to 0.5
- out_gate: bfloat16 [512, 128], P('unit'), parts along dimension 0, may hold values from -0.5 to 0.5
Outputs:
- triangle_out: bfloat16 [256, 64, 128], P(('unit', 'north'), 'east'), parts along dimension 0
The draws below stay inside these ranges and needn't reach their ends.
There are 4 independent parts, one for each index of `unit`. The reference program is written for one: setup_inputs(seed, part) draws one part's arguments, and reference() takes and returns one part's arrays. A program takes and returns all parts, laid end to end along the dimension named above; an argument that names none is the same for every part. Nothing has to cross between parts.
All inputs are finite; a program needn't handle non-finite values.
Results may differ from the reference program's by a relative error of at most 0.015.
Values may be sent and summed in bfloat16 or wider, within the bound.
A program may use at most 128 MiB of HBM per device.

```python
import jax
import jax.numpy as jnp
from jax import lax

RESIDUES = 64
PAIR_WIDTH = 128
MIX_WIDTH = 128


def block_scale(rng, dims, split, low, top_value):
    def one(position, shards_of):
        steps = jax.random.uniform(jax.random.fold_in(jax.random.fold_in(rng, 6), position), (shards_of,), jnp.float32, low / len(split), top_value / len(split))
        return jnp.repeat(jnp.exp(steps), dims[position] // shards_of).reshape((-1,) + (1,) * (len(dims) - position - 1))

    gain = one(*split[0])
    for cut in split[1:]:
        gain = gain * one(*cut)
    return gain


def scatter_about(own_key, extent, spread, reach, pieces=(), kind=jnp.bfloat16):
    values = jax.random.normal(own_key, extent, jnp.float32) * spread
    if len(pieces) > 0:
        values = block_scale(own_key, extent, pieces, -0.22, 0.18) * values
    return jnp.clip(values, min=-reach, max=reach).astype(kind)


def setup_inputs(seed: int = 0, part: int = 0) -> dict:
    key_of = jax.random.split(jax.random.key(seed), 10)
    own_keys = jax.random.split(jax.random.fold_in(key_of[9], part), 10)
    pair_rows = scatter_about(own_keys[0], (RESIDUES, RESIDUES, PAIR_WIDTH), 1.0, 6.0, ((0, 4), (1, 2)))
    in_gain = jnp.clip(1.0 + 0.15 * jax.random.normal(key_of[1], (PAIR_WIDTH,), jnp.float32), 0.25, 1.75)
    left_weight = scatter_about(own_keys[2], (PAIR_WIDTH, MIX_WIDTH), PAIR_WIDTH ** -0.5, 0.5)
    right_weight = scatter_about(own_keys[3], (PAIR_WIDTH, MIX_WIDTH), PAIR_WIDTH ** -0.5, 0.5)
    left_gate = scatter_about(own_keys[4], (PAIR_WIDTH, MIX_WIDTH), PAIR_WIDTH ** -0.5, 0.5)
    right_gate = scatter_about(own_keys[5], (PAIR_WIDTH, MIX_WIDTH), PAIR_WIDTH ** -0.5, 0.5)
    mid_gain = jnp.clip(1.0 + 0.15 * jax.random.normal(key_of[6], (MIX_WIDTH,), jnp.float32), 0.25, 1.75)
    out_weight = scatter_about(own_keys[7], (MIX_WIDTH, PAIR_WIDTH), MIX_WIDTH ** -0.5, 0.5)
    out_gate = scatter_about(own_keys[8], (PAIR_WIDTH, PAIR_WIDTH), PAIR_WIDTH ** -0.5, 0.5)
    return {"pair_rows": pair_rows, "in_gain": in_gain, "left_weight": left_weight, "right_weight": right_weight, "left_gate": left_gate, "right_gate": right_gate, "mid_gain": mid_gain, "out_weight": out_weight, "out_gate": out_gate}


def scale_channels(values, channel_gain):
    centred = values - lax.optimization_barrier(jnp.mean(values, axis=-1, keepdims=True))
    return centred * lax.rsqrt(lax.optimization_barrier(jnp.mean(centred * centred, axis=-1, keepdims=True)) + 1e-05) * channel_gain

def make_factors(pair_in, in_gain, left_weight, right_weight, left_gate, right_gate):
    ready = scale_channels(pair_in.astype(jnp.float32), in_gain).astype(jnp.bfloat16)
    ready = lax.optimization_barrier(ready)
    left = jnp.einsum('ijc,cd->ijd', ready.astype(jnp.float32), left_weight.astype(jnp.float32))
    left = left * jax.nn.sigmoid(jnp.einsum('ijc,cd->ijd', ready.astype(jnp.float32), left_gate.astype(jnp.float32)))
    right = jnp.einsum('ijc,cd->ijd', ready.astype(jnp.float32), right_weight.astype(jnp.float32))
    right = right * jax.nn.sigmoid(jnp.einsum('ijc,cd->ijd', ready.astype(jnp.float32), right_gate.astype(jnp.float32)))
    return (ready, left.astype(jnp.bfloat16), right.astype(jnp.bfloat16))

def finish_pair(mixed, ready, mid_gain, out_weight, out_gate):
    scaled = scale_channels(mixed.astype(jnp.float32), mid_gain).astype(jnp.bfloat16)
    scaled = lax.optimization_barrier(scaled)
    gate = jax.nn.sigmoid(jnp.einsum('ijc,cd->ijd', ready.astype(jnp.float32), out_gate.astype(jnp.float32)))
    return (jnp.einsum('ijd,dc->ijc', scaled.astype(jnp.float32), out_weight.astype(jnp.float32)) * gate).astype(jnp.bfloat16)

def reference(pair_rows, in_gain, left_weight, right_weight, left_gate, right_gate, mid_gain, out_weight, out_gate):
    ready, left, right = make_factors(pair_rows, in_gain, left_weight, right_weight, left_gate, right_gate)
    left, right = lax.optimization_barrier((left, right))

    def one_channel(pair_of):
        return (jnp.dot(pair_of[0].T, pair_of[1], preferred_element_type=jnp.float32) * RESIDUES ** (-0.5)).astype(jnp.bfloat16)
    mixed = jnp.moveaxis(lax.map(one_channel, (jnp.moveaxis(left, -1, 0), jnp.moveaxis(right, -1, 0))), 0, -1)
    mixed = lax.optimization_barrier(mixed)
    return finish_pair(mixed, ready, mid_gain, out_weight, out_gate)
```

```python
import functools

import jax
import jax.numpy as jnp
from jax import lax
from jax.experimental import pallas as pl
from jax.experimental.pallas import tpu as pltpu
from jax.sharding import PartitionSpec as P


def over_all(piece, axis, dim, apply):
    everything = lax.all_gather(piece, axis, axis=dim, tiled=True)
    return apply(everything, jnp.int32(0))


def scale_channels(values, channel_gain):
    centred = values - jnp.mean(values, axis=-1, keepdims=True)
    return (
        centred
        * lax.rsqrt(jnp.mean(centred * centred, axis=-1, keepdims=True) + 1e-05)
        * channel_gain
    )


def make_factors(pair_in, in_gain, left_weight, right_weight, left_gate, right_gate):
    ready = scale_channels(pair_in.astype(jnp.float32), in_gain).astype(jnp.bfloat16)
    ready = lax.optimization_barrier(ready)
    left = jnp.einsum("ijc,cd->ijd", ready, left_weight, preferred_element_type=jnp.float32)
    left = left * jax.nn.sigmoid(
        jnp.einsum("ijc,cd->ijd", ready, left_gate, preferred_element_type=jnp.float32)
    )
    right = jnp.einsum("ijc,cd->ijd", ready, right_weight, preferred_element_type=jnp.float32)
    right = right * jax.nn.sigmoid(
        jnp.einsum("ijc,cd->ijd", ready, right_gate, preferred_element_type=jnp.float32)
    )
    return (ready, left.astype(jnp.bfloat16), right.astype(jnp.bfloat16))


def finish_pair(mixed, ready, mid_gain, out_weight, out_gate):
    scaled = scale_channels(mixed.astype(jnp.float32), mid_gain).astype(jnp.bfloat16)
    scaled = lax.optimization_barrier(scaled)
    gate = jax.nn.sigmoid(
        jnp.einsum("ijc,cd->ijd", ready, out_gate, preferred_element_type=jnp.float32)
    )
    return (
        jnp.einsum("ijd,dc->ijc", scaled, out_weight, preferred_element_type=jnp.float32) * gate
    ).astype(jnp.bfloat16)


def body(
    pair_rows,
    in_gain,
    left_weight,
    right_weight,
    left_gate,
    right_gate,
    mid_gain,
    out_weight,
    out_gate,
):
    ready, left, right = make_factors(
        pair_rows, in_gain, left_weight, right_weight, left_gate, right_gate
    )
    count = pair_rows.shape[0] * lax.axis_size("north")
    left_lines, right_lines = (
        lax.all_to_all(left, "north", split_axis=2, concat_axis=0, tiled=True),
        lax.all_to_all(right, "north", split_axis=2, concat_axis=0, tiled=True),
    )

    def meet(piece, start):
        return jnp.einsum("kid,kjd->ijd", piece, right_lines, preferred_element_type=jnp.float32)

    strip = over_all(left_lines, "east", 1, meet)
    strip = (strip * count ** (-0.5)).astype(jnp.bfloat16)
    mixed = lax.all_to_all(strip, "north", split_axis=0, concat_axis=2, tiled=True)
    return finish_pair(mixed, ready, mid_gain, out_weight, out_gate)


F32 = jnp.float32
BF16 = jnp.bfloat16
MESH = pl.DeviceIdType.MESH
CHUNKS = 2
GROUP = 8


def logistic(values):
    return 0.5 * jnp.tanh(0.5 * values) + 0.5


def product(a, b):
    return jnp.dot(a, b, preferred_element_type=F32)


def fused_kernel(
    north,
    east,
    pair_ref,
    in_gain_ref,
    left_weight_ref,
    right_weight_ref,
    left_gate_ref,
    right_gate_ref,
    mid_gain_ref,
    out_weight_ref,
    out_gate_ref,
    out_ref,
    left_own,
    left_lines,
    right_lines,
    left_wide,
    right_wide,
    total,
    gate_ref,
    up_send,
    down_send,
    right_recv,
    left_send,
    left_recv,
    pass_send,
):
    lines, cols, channels = pair_ref.shape
    mix = left_weight_ref.shape[1]
    blocks = cols // lines
    n = lax.axis_index("north")
    e = lax.axis_index("east")
    partner = 1 - e
    owner = n // blocks == e
    half = lines // CHUNKS

    barrier = pltpu.get_barrier_semaphore()
    for flat in range(1, north * east):
        other_n = lax.rem(n + flat // east, north)
        other_e = lax.rem(e + flat % east, east)
        pl.semaphore_signal(
            barrier, inc=1, device_id={"north": other_n, "east": other_e}, device_id_type=MESH
        )

    rows = pair_ref[...].reshape(lines * cols, channels).astype(F32)
    ready = scale_channels(rows, in_gain_ref[...]).astype(BF16)
    right = product(ready, right_weight_ref[...]) * logistic(product(ready, right_gate_ref[...]))
    right_lines[n] = right.astype(BF16).reshape(lines, cols, mix)
    left = product(ready, left_weight_ref[...]) * logistic(product(ready, left_gate_ref[...]))
    left = left.astype(BF16).reshape(lines, blocks, lines, mix)
    for h in range(blocks):
        left_own[h] = left[:, h]

    pl.semaphore_wait(barrier, north * east - 1)

    def line_copy(source, chunk, sends, target):
        ref = right_lines.at[source, pl.ds(chunk * half, half)]
        return pltpu.make_async_remote_copy(
            src_ref=ref,
            dst_ref=ref,
            send_sem=sends.at[source, chunk],
            recv_sem=right_recv.at[source, chunk],
            device_id={"north": target},
            device_id_type=MESH,
        )

    def up_copy(source, chunk):
        return line_copy(source, chunk, up_send, jnp.minimum(n + 1, north - 1))

    def down_copy(source, chunk):
        return line_copy(source, chunk, down_send, jnp.maximum(n - 1, 0))

    def left_copy(h):
        return pltpu.make_async_remote_copy(
            src_ref=left_own.at[h],
            dst_ref=left_lines.at[n],
            send_sem=left_send.at[h],
            recv_sem=left_recv.at[n],
            device_id={"north": e * blocks + h},
            device_id_type=MESH,
        )

    def own_pass(h):
        return pltpu.make_async_remote_copy(
            src_ref=left_own.at[h],
            dst_ref=left_lines.at[n],
            send_sem=pass_send.at[n],
            recv_sem=left_recv.at[n],
            device_id={"east": partner},
            device_id_type=MESH,
        )

    def pass_copy(source):
        return pltpu.make_async_remote_copy(
            src_ref=left_lines.at[source],
            dst_ref=left_lines.at[source],
            send_sem=pass_send.at[source],
            recv_sem=left_recv.at[source],
            device_id={"east": partner},
            device_id_type=MESH,
        )

    for chunk in range(CHUNKS):
        @pl.when(n < north - 1)
        def _():
            up_copy(n, chunk).start()

        @pl.when(n > 0)
        def _():
            down_copy(n, chunk).start()

    for h in range(blocks):
        @pl.when(e * blocks + h == n)
        def _():
            own_pass(h).start()
            left_lines[n] = left_own[h]

        @pl.when(e * blocks + h != n)
        def _():
            left_copy(h).start()

    gate_ref[...] = logistic(product(ready, out_gate_ref[...]))
    total[...] = jnp.zeros_like(total)

    def contract(source):
        left_wide[...] = left_lines[source].astype(F32)
        right_wide[...] = right_lines[source].astype(F32)

        def group(g, carry):
            base = pl.multiple_of(g * GROUP, GROUP)
            sums = [total[base + i] for i in range(GROUP)]
            for k in range(lines):
                r = right_wide[k]
                for i in range(GROUP):
                    row = left_wide[k, pl.ds(base + i, 1), :]
                    sums[i] = sums[i] + jnp.broadcast_to(row, r.shape) * r
            for i in range(GROUP):
                total[base + i] = sums[i]
            return carry

        lax.fori_loop(0, lines // GROUP, group, 0)

    @pl.when(jnp.logical_not(owner))
    def _():
        pass_copy(n).wait_recv()

    contract(n)

    for step in range(1, north):
        below, above = n - step, n + step
        for chunk in range(CHUNKS):
            @pl.when(below >= 0)
            def _():
                up_copy(below, chunk).wait_recv()

                @pl.when(n < north - 1)
                def _():
                    up_copy(below, chunk).start()

            @pl.when(above < north)
            def _():
                down_copy(above, chunk).wait_recv()

                @pl.when(n > 0)
                def _():
                    down_copy(above, chunk).start()

        for source in (below, above):
            @pl.when(jnp.logical_and(source >= 0, source < north))
            def _():
                pass_copy(source).wait_recv()

                @pl.when(owner)
                def _():
                    pass_copy(source).start()

        for source in (below, above):
            @pl.when(jnp.logical_and(source >= 0, source < north))
            def _():
                contract(source)

    mixed = (total[...] * (lines * north) ** (-0.5)).astype(BF16).astype(F32)
    mixed = mixed.reshape(lines * cols, mix)
    scaled = scale_channels(mixed, mid_gain_ref[...]).astype(BF16)
    out = product(scaled, out_weight_ref[...]) * gate_ref[...]
    out_ref[...] = out.astype(BF16).reshape(lines, cols, channels)

    for h in range(blocks):
        @pl.when(e * blocks + h == n)
        def _():
            own_pass(h).wait_send()

        @pl.when(e * blocks + h != n)
        def _():
            left_copy(h).wait_send()

    for source in range(north):
        @pl.when(jnp.logical_and(owner, source != n))
        def _():
            pass_copy(source).wait_send()

        for chunk in range(CHUNKS):
            @pl.when(jnp.logical_and(source <= n, n < north - 1))
            def _():
                up_copy(source, chunk).wait_send()

            @pl.when(jnp.logical_and(source >= n, n > 0))
            def _():
                down_copy(source, chunk).wait_send()


def fused_body(
    pair_rows,
    in_gain,
    left_weight,
    right_weight,
    left_gate,
    right_gate,
    mid_gain,
    out_weight,
    out_gate,
):
    north, east = lax.axis_size("north"), lax.axis_size("east")
    lines, cols, channels = pair_rows.shape
    mix = left_weight.shape[1]
    blocks = cols // lines
    vmem = pl.BlockSpec(memory_space=pltpu.VMEM)
    dma = pltpu.SemaphoreType.DMA
    return pl.pallas_call(
        functools.partial(fused_kernel, north, east),
        out_shape=jax.ShapeDtypeStruct(pair_rows.shape, BF16),
        in_specs=[vmem] * 9,
        out_specs=vmem,
        scratch_shapes=[
            pltpu.VMEM((blocks, lines, lines, mix), BF16),
            pltpu.VMEM((north, lines, lines, mix), BF16),
            pltpu.VMEM((north, lines, cols, mix), BF16),
            pltpu.VMEM((lines, lines, mix), F32),
            pltpu.VMEM((lines, cols, mix), F32),
            pltpu.VMEM((lines, cols, mix), F32),
            pltpu.VMEM((lines * cols, channels), F32),
            dma((north, CHUNKS)),
            dma((north, CHUNKS)),
            dma((north, CHUNKS)),
            dma((blocks,)),
            dma((north,)),
            dma((north,)),
        ],
        compiler_params=pltpu.CompilerParams(collective_id=0, has_side_effects=True),
    )(
        pair_rows,
        in_gain.reshape(1, -1),
        left_weight,
        right_weight,
        left_gate,
        right_gate,
        mid_gain.reshape(1, -1),
        out_weight,
        out_gate,
    )


def choose_body(*args):
    lines, cols, channels = args[0].shape
    north, east = lax.axis_size("north"), lax.axis_size("east")
    small = north * lines * (lines + cols) * args[2].shape[1] <= 2**21
    if small and east == 2 and lines * north == cols * east and lines % 16 == 0:
        return fused_body(*args)
    return body(*args)


def solution(mesh):
    placed = (
        P(("unit", "north"), "east", None),
        P(),
        P("unit", None),
        P("unit", None),
        P("unit", None),
        P("unit", None),
        P(),
        P("unit", None),
        P("unit", None),
    )
    return jax.shard_map(
        choose_body,
        mesh=mesh,
        in_specs=placed,
        out_specs=P(("unit", "north"), "east", None),
        check_vma=False,
    )
```
